32 devices in a mesh: seq: 4 (over y, core), head: 8 (over z, x).
Axes of the slice: x: 2, y: 2, z: 4, core: 2. Of those that a mesh axis runs over, the one named last changes fastest.
Arguments:
- tokens: bfloat16 [3072, 8192], P('seq', 'head'), may hold values from -6 to 6
- w_query: bfloat16 [8192, 8192], P(None, 'head'), may hold values from -0.0625 to 0.0625
- w_key: bfloat16 [8192, 1024], P(None, 'head'), may hold values from -0.0625 to 0.0625
- w_value: bfloat16 [8192, 1024], P(None, 'head'), may hold values from -0.0625 to 0.0625
- map_query: float32 [64, 128, 64], P('head'), may hold values from -0.5 to 0.5
- map_key: float32 [64, 128, 64], P('head'), may hold values from -0.5 to 0.5
Outputs:
- student_out: bfloat16 [3072, 8192], P('seq', 'head')
- grad_query_map: float32 [64, 128, 64], P('head')
- grad_key_map: float32 [64, 128, 64], P('head')
The draws below stay inside these ranges and needn't reach their ends.
All inputs are finite; a program needn't handle non-finite values.
Results may differ from the reference program's by a relative error of at most 0.013.
Values may be sent and summed in bfloat16 or wider, within the bound.
A program may use at most 128 MiB of HBM per device.

```python
import math
import jax
import jax.numpy as jnp
from jax import lax

D = 8192
HEADS = 64
KVH = 8
DH = 128
FEAT = 64
TOKENS = 3072


def block_levels(rng, shape, shards, smallest, largest):
    factor_of = 1.0
    for position, blocks in shards:
        heights = jax.random.uniform(jax.random.fold_in(jax.random.fold_in(rng, 6), position), (blocks,), jnp.float32, smallest / len(shards), largest / len(shards))
        factor_of = factor_of * jnp.repeat(jnp.exp(heights), shape[position] // blocks).reshape((-1,) + (1,) * (len(shape) - 1 - position))
    return factor_of


def gaussian(key, dims, deviation, limit, shards=(), held_as=jnp.bfloat16):
    loudness = block_levels(key, dims, shards, -0.22, 0.18) if shards else 1.0
    entries = jax.random.normal(key, dims, jnp.float32) * deviation * loudness
    return jnp.minimum(jnp.maximum(entries, -limit), limit).astype(held_as)


def setup_inputs(seed: int = 0) -> dict:
    seeds = jax.random.split(jax.random.key(seed), 7)
    tokens = gaussian(seeds[0], (TOKENS, D), 1.0, 6.0, ((0, 4), (1, 8)))
    w_query = gaussian(seeds[1], (D, HEADS * DH), D ** -0.5, 0.0625, ((1, 8),))
    w_key = gaussian(seeds[2], (D, KVH * DH), D ** -0.5, 0.0625, ((1, 8),))
    w_value = gaussian(seeds[3], (D, KVH * DH), D ** -0.5, 0.0625, ((1, 8),))
    map_query = gaussian(seeds[4], (HEADS, DH, FEAT), DH ** -0.5, 0.5, ((0, 8),), jnp.float32)
    map_key = gaussian(seeds[5], (HEADS, DH, FEAT), DH ** -0.5, 0.5, ((0, 8),), jnp.float32)
    return dict(tokens=tokens, w_query=w_query, w_key=w_key, w_value=w_value, map_query=map_query, map_key=map_key)


ROPE_BASE = 500000.0
MATMUL_ACCURACY = lax.Precision.HIGHEST

def rope_tables(length, width, offset):
    half_width = width // 2
    positions = (offset + jnp.arange(length)).astype(jnp.float32)
    exponent = jnp.arange(half_width).astype(jnp.float32) * (2.0 / width)
    frequency = jnp.power(jnp.float32(ROPE_BASE), -exponent)
    angles = positions[:, None] * frequency[None, :]
    return (jnp.cos(angles), jnp.sin(angles))

def rotate(vectors, cosine, sine):
    half_width = vectors.shape[-1] // 2
    first = vectors[..., :half_width]
    second = vectors[..., half_width:]
    cosine = cosine[:, None, :]
    sine = sine[:, None, :]
    return jnp.concatenate([first * cosine - second * sine, second * cosine + first * sine], axis=-1)

def feature_map(vectors, weights):
    logits = jnp.einsum('thd,hdf->thf', vectors, weights, precision=MATMUL_ACCURACY)
    upper = jnp.exp(logits)
    lower = jnp.exp(-logits)
    return jnp.concatenate([upper / lax.optimization_barrier(jnp.sum(upper, -1, keepdims=True)), lower / lax.optimization_barrier(jnp.sum(lower, -1, keepdims=True))], axis=-1)

def reference(tokens, w_query, w_key, w_value, map_query, map_key):
    length = tokens.shape[0]
    group = HEADS // KVH
    query_rows = jnp.dot(tokens, w_query, preferred_element_type=jnp.float32).reshape(length, HEADS, DH)
    keys = jnp.dot(tokens, w_key, preferred_element_type=jnp.float32).astype(jnp.bfloat16)
    values = jnp.dot(tokens, w_value, preferred_element_type=jnp.float32).astype(jnp.bfloat16)
    cosine, sine = rope_tables(length, DH, 0)
    queries_rot = rotate(query_rows, cosine, sine).astype(jnp.bfloat16)
    keys_rot = rotate(keys.astype(jnp.float32).reshape(length, KVH, DH), cosine, sine).astype(jnp.bfloat16)
    values = values.reshape(length, KVH, DH)
    causal = jnp.arange(length)[None, :] <= jnp.arange(length)[:, None]
    query_head_count = jnp.transpose(queries_rot, (1, 0, 2))
    key_heads = jnp.transpose(keys_rot, (1, 0, 2))
    value_heads = jnp.transpose(values, (1, 0, 2))
    scale = 1.0 / math.sqrt(DH)

    def teacher_head(index):
        shared_index = index // group
        scores = jnp.dot(query_head_count[index], key_heads[shared_index].T, preferred_element_type=jnp.float32) * scale
        weights = jnp.exp(jnp.where(causal, scores, -1e+30))
        total = lax.optimization_barrier(jnp.sum(weights, -1))
        mixed = jnp.dot(weights.astype(jnp.bfloat16), value_heads[shared_index], preferred_element_type=jnp.float32)
        return (mixed / total[:, None]).astype(jnp.bfloat16)
    teacher = lax.map(teacher_head, jnp.arange(HEADS))
    target = jnp.transpose(teacher, (1, 0, 2)).astype(jnp.float32)
    keys_wide = jnp.repeat(keys_rot.astype(jnp.float32), group, axis=1)
    value_rows_broad = jnp.transpose(jnp.repeat(values.astype(jnp.float32), group, axis=1), (1, 0, 2))
    query_float = queries_rot.astype(jnp.float32)
    mask = causal.astype(jnp.float32)

    def student_head(inputs):
        query_feature_rows, key_feature_rows, head_values = inputs
        within = jnp.dot(query_feature_rows, key_feature_rows.T, precision=MATMUL_ACCURACY) * mask
        numerator = jnp.dot(within, head_values, precision=MATMUL_ACCURACY)
        return numerator / lax.optimization_barrier(jnp.sum(within, -1))[:, None]

    def student(query_weights, key_weights):
        query_features = jnp.transpose(feature_map(query_float, query_weights), (1, 0, 2))
        key_features = jnp.transpose(feature_map(keys_wide, key_weights), (1, 0, 2))
        outputs = lax.map(jax.checkpoint(student_head), (query_features, key_features, value_rows_broad))
        outputs = jnp.transpose(outputs, (1, 0, 2))
        loss = jnp.sum((outputs - target) ** 2)
        return (loss, outputs)
    loss, pullback, outputs = jax.vjp(student, map_query, map_key, has_aux=True)
    grad_query_map, grad_key_map = pullback(jnp.ones_like(loss))
    student_out = outputs.astype(jnp.bfloat16).reshape(length, HEADS * DH)
    return (student_out, grad_query_map, grad_key_map)
```

```python
import math

import jax
import jax.numpy as jnp
from jax import lax
from jax.experimental import pallas as pl
from jax.experimental.pallas import tpu as pltpu
from jax.sharding import PartitionSpec as P

DH = 128


ROPE_BASE = 500000.0
MATMUL_ACCURACY = lax.Precision.DEFAULT


def partner(value, axis, apart):
    mask = 2**apart
    pairs = [(source, source ^ mask) for source in range(lax.axis_size(axis))]
    return lax.ppermute(value, axis, pairs)


def rope_tables(length, width, offset):
    half_width = width // 2
    positions = (offset + jnp.arange(length)).astype(jnp.float32)
    exponent = jnp.arange(half_width).astype(jnp.float32) * (2.0 / width)
    frequency = jnp.power(jnp.float32(ROPE_BASE), -exponent)
    angles = positions[:, None] * frequency[None, :]
    return (jnp.cos(angles), jnp.sin(angles))


def rotate(vectors, cosine, sine):
    half_width = vectors.shape[-1] // 2
    first = vectors[..., :half_width]
    second = vectors[..., half_width:]
    cosine = cosine[:, None, :]
    sine = sine[:, None, :]
    return jnp.concatenate(
        [first * cosine - second * sine, second * cosine + first * sine], axis=-1
    )


def feature_map(vectors, weights):
    logits = jnp.einsum("thd,hdf->thf", vectors, weights, precision=MATMUL_ACCURACY)
    upper = jnp.exp(logits)
    lower = jnp.exp(-logits)
    return jnp.concatenate(
        [upper / jnp.sum(upper, -1, keepdims=True), lower / jnp.sum(lower, -1, keepdims=True)],
        axis=-1,
    )


def teacher_kernel(first_ref, query_ref, key_ref, value_ref, out_ref):
    rows = query_ref.shape[0]
    block = rows // 2 if rows % 2 == 0 else rows
    first = first_ref[0]
    scale = 1.0 / math.sqrt(query_ref.shape[1])
    queries = query_ref[...]

    def scored(start):
        keys = key_ref[pl.ds(start, block), :]
        scores = lax.dot_general(
            queries, keys, (((1,), (1,)), ((), ())), preferred_element_type=jnp.float32
        )
        return scores * scale

    def add(carry, weights, start):
        numerator, denominator = carry
        values = value_ref[pl.ds(start, block), :]
        denominator = denominator + jnp.sum(weights, axis=1, keepdims=True)
        numerator = numerator + jnp.dot(
            weights.astype(jnp.bfloat16), values, preferred_element_type=jnp.float32
        )
        return numerator, denominator

    def earlier(index, carry):
        start = pl.multiple_of(index * block, block)
        return add(carry, jnp.exp(scored(start)), start)

    carry = (
        jnp.zeros((rows, out_ref.shape[1]), jnp.float32),
        jnp.zeros((rows, 1), jnp.float32),
    )
    carry = lax.fori_loop(0, first // block, earlier, carry)
    for part in range(rows // block):
        start = pl.multiple_of(first + part * block, block)
        row = lax.broadcasted_iota(jnp.int32, (rows, block), 0)
        column = lax.broadcasted_iota(jnp.int32, (rows, block), 1) + part * block
        weights = jnp.exp(jnp.where(column <= row, scored(start), -1e30))
        carry = add(carry, weights, start)
    numerator, denominator = carry
    out_ref[...] = (numerator / denominator).astype(out_ref.dtype)


def teacher_attention(first, queries_rot, keys_rot, values):
    rows, width = queries_rot.shape
    span = keys_rot.shape[0]
    return pl.pallas_call(
        teacher_kernel,
        out_shape=jax.ShapeDtypeStruct((rows, width), jnp.bfloat16),
        grid_spec=pltpu.PrefetchScalarGridSpec(
            num_scalar_prefetch=1,
            grid=(width // DH,),
            in_specs=[
                pl.BlockSpec((rows, DH), lambda head, first: (0, head)),
                pl.BlockSpec((span, DH), lambda head, first: (0, 0)),
                pl.BlockSpec((span, DH), lambda head, first: (0, 0)),
            ],
            out_specs=pl.BlockSpec((rows, DH), lambda head, first: (0, head)),
        ),
        compiler_params=pltpu.CompilerParams(vmem_limit_bytes=32 * 1024 * 1024),
        cost_estimate=pl.CostEstimate(
            flops=4 * rows * span * width,
            bytes_accessed=4 * rows * width + 4 * span * DH,
            transcendentals=rows * span * (width // DH),
        ),
    )(jnp.reshape(first, (1,)).astype(jnp.int32), queries_rot, keys_rot, values)


def from_lower(value, shift):
    size = lax.axis_size("seq")
    return lax.ppermute(value, "seq", [(i, i + shift) for i in range(size - shift)])


def from_higher(value, shift):
    size = lax.axis_size("seq")
    return lax.ppermute(value, "seq", [(i + shift, i) for i in range(size - shift)])


def sum_of_others(arrays, receive):
    totals = [jnp.zeros(array.shape, jnp.float32) for array in arrays]
    for shift in range(1, lax.axis_size("seq")):
        for slot, array in enumerate(arrays):
            totals[slot] = totals[slot] + receive(array, shift).astype(jnp.float32)
    return totals


def gather_seq(piece):
    size = lax.axis_size("seq")
    rows = piece.shape[0]
    me = lax.axis_index("seq")
    whole = jnp.zeros((size * rows,) + piece.shape[1:], piece.dtype)
    whole = lax.dynamic_update_slice_in_dim(whole, piece, me * rows, 0)
    for shift in range(1, size):
        source = (me - shift + size) % size
        got = lax.ppermute(piece, "seq", [(i, (i + shift) % size) for i in range(size)])
        whole = lax.dynamic_update_slice_in_dim(whole, got, source * rows, 0)
    return whole


def token_blocks(tokens):
    size = lax.axis_size("head")
    me = lax.axis_index("head")
    if size != 8:
        gathered = lax.all_gather(tokens, "head", axis=1, tiled=True)
        return [(jnp.int32(0), gathered)]
    ring = size // 2
    z, x = me // 2, me % 2

    def up(value):
        return lax.ppermute(value, "head", [(s, (s + 2) % size) for s in range(size)])

    def down(value):
        return lax.ppermute(value, "head", [(s, (s + size - 2) % size) for s in range(size)])

    def across(value):
        return lax.ppermute(value, "head", [(s, s ^ 1) for s in range(size)])

    def index(dz, dx):
        return ((z + dz) % ring) * 2 + (x + dx) % 2

    half = tokens.shape[0] // 2
    below = up(tokens)
    above = down(tokens)
    beside = across(tokens)
    far = jnp.concatenate([up(below[:half]), down(above[half:])], 0)
    beside_below = up(beside)
    beside_above = down(beside)
    beside_far = across(far)
    return [
        (index(0, 0), tokens),
        (index(0, 1), beside),
        (index(ring - 1, 0), below),
        (index(1, 0), above),
        (index(2, 0), far),
        (index(ring - 1, 1), beside_below),
        (index(1, 1), beside_above),
        (index(2, 1), beside_far),
    ]


def per_device(tokens, w_query, w_key, w_value, map_query, map_key):
    row_count = tokens.shape[0]
    head_count = w_query.shape[1] // DH
    shared_width = w_key.shape[1]
    w_pair = jnp.concatenate([w_key, w_value], 1)
    query_rows = jnp.zeros((row_count, w_query.shape[1]), jnp.float32)
    pair_rows = jnp.zeros((row_count, w_pair.shape[1]), jnp.float32)
    for position, block in token_blocks(tokens):
        depth = block.shape[1]
        weights = lax.dynamic_slice_in_dim(w_query, position * depth, depth, 0)
        pair_weights = lax.dynamic_slice_in_dim(w_pair, position * depth, depth, 0)
        query_rows = query_rows + jnp.dot(block, weights, preferred_element_type=jnp.float32)
        pair_rows = pair_rows + jnp.dot(block, pair_weights, preferred_element_type=jnp.float32)
    keys = pair_rows[:, :shared_width]
    values = pair_rows[:, shared_width:]
    keys = keys.astype(jnp.bfloat16)
    values = values.astype(jnp.bfloat16)
    if shared_width < DH:
        partner_keys, partner_values = partner((keys, values), "head", 0)
        upper_half = lax.axis_index("head") % 2 == 1
        keys = jnp.where(
            upper_half,
            jnp.concatenate([partner_keys, keys], 1),
            jnp.concatenate([keys, partner_keys], 1),
        )
        values = jnp.where(
            upper_half,
            jnp.concatenate([partner_values, values], 1),
            jnp.concatenate([values, partner_values], 1),
        )
    chain_index = lax.axis_index("seq")
    query_first = chain_index * row_count
    cosine, sine = rope_tables(row_count, DH, query_first)
    queries_rot = rotate(query_rows.reshape(row_count, head_count, DH), cosine, sine).astype(
        jnp.bfloat16
    )
    keys_rot = (
        rotate(keys.astype(jnp.float32).reshape(row_count, 1, DH), cosine, sine)
        .reshape(row_count, DH)
        .astype(jnp.bfloat16)
    )
    pair_all = gather_seq(jnp.concatenate([keys_rot, values], 1))
    teacher = teacher_attention(
        query_first,
        queries_rot.reshape(row_count, head_count * DH),
        pair_all[:, :DH],
        pair_all[:, DH:],
    )
    query_float = queries_rot.astype(jnp.float32)
    key_float = jnp.broadcast_to(
        keys_rot.astype(jnp.float32)[:, None, :], (row_count, head_count, DH)
    )
    value_single_float = values.astype(jnp.float32)
    query_features = feature_map(query_float, map_query)
    key_features = feature_map(key_float, map_key)
    state_local = jnp.einsum(
        "thf,td->hfd", key_features, value_single_float, precision=MATMUL_ACCURACY
    )
    norm_local = jnp.sum(key_features, 0)
    state_before, norm_before = sum_of_others(
        (state_local.astype(jnp.bfloat16), norm_local), from_lower
    )
    local_mask = (jnp.arange(row_count)[None, :] <= jnp.arange(row_count)[:, None]).astype(
        jnp.float32
    )

    def student_local(query_feature_rows, key_feature_rows, state, norm):
        within = (
            jnp.einsum(
                "ueo,aeo->eua", query_feature_rows, key_feature_rows, precision=MATMUL_ACCURACY
            )
            * local_mask[None]
        )
        upper = jnp.einsum("hqk,kd->qhd", within, value_single_float, precision=MATMUL_ACCURACY)
        upper = upper + jnp.einsum(
            "qhf,hfd->qhd", query_feature_rows, state, precision=MATMUL_ACCURACY
        )
        lower = jnp.transpose(jnp.sum(within, -1)) + jnp.einsum(
            "qhf,hf->qh", query_feature_rows, norm, precision=MATMUL_ACCURACY
        )
        return upper / lower[..., None]

    student, pullback = jax.vjp(
        student_local, query_features, key_features, state_before, norm_before
    )
    student_out = student.astype(jnp.bfloat16).reshape(row_count, head_count * DH)
    target = teacher.reshape(row_count, head_count, DH).astype(jnp.float32)
    grad_student = 2.0 * (student - target)
    grad_query_feat, grad_key_feat, grad_state, grad_norm = pullback(grad_student)
    state_after, norm_after = sum_of_others(
        (grad_state.astype(jnp.bfloat16), grad_norm), from_higher
    )
    grad_key_feat = (
        grad_key_feat
        + jnp.einsum("td,hfd->thf", value_single_float, state_after, precision=MATMUL_ACCURACY)
        + norm_after[None]
    )
    unused_query, query_backward = jax.vjp(
        lambda weights: feature_map(query_float, weights), map_query
    )
    unused_key, pull_key = jax.vjp(lambda weights: feature_map(key_float, weights), map_key)
    grad_query = query_backward(grad_query_feat)[0]
    grad_key = pull_key(grad_key_feat)[0]
    features = grad_query.shape[-1]
    grads = jnp.concatenate([grad_query, grad_key], -1)
    size = lax.axis_size("seq")
    if size & (size - 1):
        grads = lax.psum(grads, "seq")
    else:
        apart = 0
        while 2**apart < size:
            if apart > 0:
                sent = grads.astype(jnp.bfloat16)
                grads = sent.astype(jnp.float32) + partner(sent, "seq", apart).astype(jnp.float32)
            else:
                grads = grads + partner(grads, "seq", apart)
            apart += 1
    grad_query, grad_key = grads[..., :features], grads[..., features:]
    return (student_out, grad_query, grad_key)


def solution(mesh):
    in_specs = (
        P("seq", "head"),
        P(None, "head"),
        P(None, "head"),
        P(None, "head"),
        P("head", None, None),
        P("head", None, None),
    )
    out_specs = (P("seq", "head"), P("head", None, None), P("head", None, None))
    return jax.shard_map(
        per_device, mesh=mesh, in_specs=in_specs, out_specs=out_specs, check_vma=False
    )
```
